32 devices in a mesh: ep: 8 (over y, x, core), dp: 4 (over z).
Axes of the slice: x: 2, y: 2, z: 4, core: 2. Of those that a mesh axis runs over, the one named last changes fastest.
Arguments:
- tokens: bfloat16 [64, 7168], P('dp', 'ep'), may hold values from -6 to 6
- norm_gain: float32 [2, 7168], replicated, may hold values from 0.1 to 1.9
- gate_weight: bfloat16 [2, 12, 2048, 7168], P(None, 'dp', 'ep'), may hold values from -0.0625 to 0.0625
- up_weight: bfloat16 [2, 12, 2048, 7168], P(None, 'dp', 'ep'), may hold values from -0.0625 to 0.0625
- down_weight: bfloat16 [2, 12, 7168, 2048], P(None, 'dp', 'ep'), may hold values from -0.125 to 0.125
- replica_plan: int32 [2, 4, 2], replicated, may hold values from 0 to 2
- route_expert: int32 [2, 64, 8], replicated, may hold values from 0 to 11, as said below
- replica_pick: int32 [2, 64, 8], replicated, may hold values from 0 to 2
- combine_num: int32 [2, 64, 8], P(None, 'dp'), may hold values from 1 to 8
Outputs:
- stream_out: bfloat16 [64, 7168], P('dp', 'ep')
- last_update: bfloat16 [64, 7168], P('dp', 'ep')
The draws below stay inside these ranges and needn't reach their ends.
Inputs may be any that keep to these rules, and one draw needn't show every extreme that they name: `route_expert`: each row of one layer names 8 different experts.
All inputs are finite; a program needn't handle non-finite values.
Results may differ from the reference program's by a relative error of at most 0.011.
Values may be sent and summed in bfloat16 or wider, within the bound.
A program may use at most 256 MiB of HBM per device.

```python
import jax
import jax.numpy as jnp
from jax import lax

D = 7168
FF = 2048
TOPK = 8
EXP_HOST = 3
REP_HOST = 2
LAYERS = 2
TOK_GRP = 16
CAP = 8
EXPERTS = 12
TOKENS = 64
N_DP = 4


def hot_choice(key):
    return jax.random.randint(jax.random.fold_in(key, 7), (LAYERS, TOKENS // TOK_GRP), 0, EXPERTS).astype(jnp.int32)


def hot_rows(key):
    hot = hot_choice(key)
    group_of = jnp.arange(TOKENS, dtype=jnp.int32) // TOK_GRP
    return hot[:, group_of]


def draw_route_expert(key, part):
    noise = jax.random.randint(jax.random.fold_in(key, 11), (LAYERS, TOKENS, EXPERTS), 0, 2 ** 18)
    favour = jax.random.randint(jax.random.fold_in(key, 13), (LAYERS, 1, EXPERTS), 0, 3) * 2 ** 18
    column = jnp.arange(EXPERTS, dtype=jnp.int32)
    boost = (column[None, None, :] == hot_rows(key)[:, :, None]).astype(jnp.int32) * 2 ** 22
    scores = (noise + favour + boost) * EXPERTS + column[None, None, :]
    values, picked = lax.top_k(scores, TOPK)
    return picked.astype(jnp.int32)


def draw_replica_pick(key, part):
    routes = draw_route_expert(key, part)
    picks = jax.random.randint(jax.random.fold_in(key, 17), (LAYERS, TOKENS, TOPK), 0, 3)
    return jnp.where(routes == hot_rows(key)[:, :, None], 0, picks).astype(jnp.int32)


def set_ends(entries, rng, low, top_value):
    longest = entries.shape.index(max(entries.shape))
    spots = []
    for shift in (0, 1):
        where = [jax.random.randint(jax.random.fold_in(rng, axis), (), 0, length) for axis, length in enumerate(entries.shape)]
        where[longest] = (where[longest] + shift) % entries.shape[longest]
        spots.append(tuple(where))
    return entries.at[spots[0]].set(low).at[spots[1]].set(top_value)


def steps_of(own_key, extent, shards, low, largest):
    factor_of = 1.0
    for dim, parts in shards:
        steps = jax.random.uniform(jax.random.fold_in(jax.random.fold_in(own_key, 6), dim), (parts,), jnp.float32, low / len(shards), largest / len(shards))
        factor_of = factor_of * jnp.repeat(jnp.exp(steps), extent[dim] // parts).reshape((-1,) + (1,) * (len(extent) - 1 - dim))
    return factor_of


def gaussian(stream_key, shape, deviation, most, shards=(), kind=jnp.bfloat16):
    values = deviation * jax.random.normal(stream_key, shape, jnp.float32)
    if shards:
        values = values * steps_of(stream_key, shape, shards, -0.22, 0.18)
    return jnp.clip(values, -most, most).astype(kind)


def setup_inputs(seed: int = 0) -> dict:
    key_list = jax.random.split(jax.random.key(seed), 10)
    tokens = gaussian(key_list[0], (TOKENS, D), 1.0, 6.0, ((0, 4), (1, 8)))
    norm_gain = jnp.clip(1.0 + 0.18 * jax.random.normal(key_list[1], (LAYERS, D), jnp.float32), 0.1, 1.9)
    gate_weight = gaussian(key_list[2], (LAYERS, EXPERTS, FF, D), D ** -0.5, 0.0625, ((1, 4), (2, 8)))
    up_weight = gaussian(key_list[3], (LAYERS, EXPERTS, FF, D), D ** -0.5, 0.0625, ((1, 4), (2, 8)))
    down_weight = gaussian(key_list[4], (LAYERS, EXPERTS, D, FF), FF ** -0.5, 0.125, ((1, 4), (2, 8)))
    replica_plan = set_ends(jax.random.randint(key_list[5], (LAYERS, N_DP, REP_HOST), 0, EXP_HOST), jax.random.fold_in(key_list[5], 1), 0, EXP_HOST - 1).astype(jnp.int32)
    route_expert = draw_route_expert(jax.random.fold_in(key_list[9], 71), 0)
    replica_pick = draw_replica_pick(jax.random.fold_in(key_list[9], 71), 0)
    combine_num = set_ends(jax.random.randint(key_list[8], (LAYERS, TOKENS, TOPK), 1, 9), jax.random.fold_in(key_list[8], 1), 1, 8).astype(jnp.int32)
    return dict(tokens=tokens, norm_gain=norm_gain, gate_weight=gate_weight, up_weight=up_weight, down_weight=down_weight, replica_plan=replica_plan, route_expert=route_expert, replica_pick=replica_pick, combine_num=combine_num)


epsilon = 1e-06

def serve_table(plan_layer):
    replicas = EXP_HOST + REP_HOST
    flat_ids = jnp.arange(N_DP * replicas, dtype=jnp.int32)
    host_of = flat_ids // replicas
    local_id = flat_ids % replicas
    copy_id = jnp.clip(local_id - EXP_HOST, 0, REP_HOST - 1)
    owner = (host_of - 1 - copy_id) % N_DP
    copied = owner * EXP_HOST + plan_layer[host_of, copy_id]
    return jnp.where(local_id < EXP_HOST, host_of * EXP_HOST + local_id, copied).astype(jnp.int32)

def targets(experts_g, picks_g, table):
    flat_e = experts_g.reshape(-1)
    flat_p = picks_g.reshape(-1)
    matches = (table[None, :] == flat_e[:, None]).astype(jnp.int32)
    counts = lax.optimization_barrier(jnp.sum(matches, axis=1))
    rank_in = jnp.cumsum(matches, axis=1) - 1
    wanted = flat_p % counts
    chosen = matches * (rank_in == wanted[:, None]).astype(jnp.int32)
    target = lax.optimization_barrier(jnp.sum(chosen * jnp.arange(table.shape[0], dtype=jnp.int32)[None, :], axis=1))
    before = jnp.cumsum(chosen, axis=0) - chosen
    position = lax.optimization_barrier(jnp.sum(before * chosen, axis=1))
    return (target.astype(jnp.int32), position.astype(jnp.int32))

def reference(tokens, norm_gain, gate_weight, up_weight, down_weight, replica_plan, route_expert, replica_pick, combine_num):
    stream = tokens
    update = jnp.zeros((TOKENS, D), jnp.float32)
    for layer_id in range(LAYERS):
        stream_f = stream.astype(jnp.float32)
        mean_sq = lax.optimization_barrier(jnp.mean(stream_f * stream_f, axis=1, keepdims=True))
        normed = (stream_f * lax.rsqrt(mean_sq + epsilon) * norm_gain[layer_id][None, :]).astype(jnp.bfloat16)

        def one_expert(weights):
            gate_act = jnp.dot(normed, weights[0].T, preferred_element_type=jnp.float32)
            up_act = jnp.dot(normed, weights[1].T, preferred_element_type=jnp.float32)
            hidden = (jax.nn.silu(gate_act) * up_act).astype(jnp.bfloat16)
            return jnp.dot(hidden, weights[2].T, preferred_element_type=jnp.float32).astype(jnp.bfloat16)
        every_out = lax.map(one_expert, (gate_weight[layer_id], up_weight[layer_id], down_weight[layer_id]))
        table = serve_table(replica_plan[layer_id])
        experts_l = route_expert[layer_id]
        grouped_e = experts_l.reshape(N_DP, TOK_GRP, TOPK)
        grouped_p = replica_pick[layer_id].reshape(N_DP, TOK_GRP, TOPK)
        target, position = jax.vmap(lambda e_blk, p_blk: targets(e_blk, p_blk, table))(grouped_e, grouped_p)
        kept_mask = (position.reshape(TOKENS, TOPK) < CAP).astype(jnp.float32)
        flat_e = experts_l.reshape(-1)
        token_ids = jnp.repeat(jnp.arange(TOKENS, dtype=jnp.int32), TOPK)
        picked = every_out[flat_e, token_ids].astype(jnp.float32).reshape(TOKENS, TOPK, D)
        numerator = combine_num[layer_id].astype(jnp.float32)
        weights_k = numerator / lax.optimization_barrier(jnp.sum(numerator, axis=1, keepdims=True))
        combine = weights_k * kept_mask
        update = lax.optimization_barrier(jnp.sum(combine[:, :, None] * picked, axis=1))
        stream = (stream.astype(jnp.float32) + update).astype(jnp.bfloat16)
    return (stream, update.astype(jnp.bfloat16))
```

```python
import jax
import jax.numpy as jnp
from jax import lax
from jax.experimental import pallas as pl
from jax.experimental.pallas import tpu as pltpu
from jax.sharding import PartitionSpec as P

import functools

epsilon = 1e-06


def serve_table(plan_layer, host_count, exp_host, rep_host):
    replicas = exp_host + rep_host
    flat_ids = jnp.arange(host_count * replicas, dtype=jnp.int32)
    host_of = flat_ids // replicas
    local_id = flat_ids % replicas
    copy_id = jnp.clip(local_id - exp_host, 0, rep_host - 1)
    owner = (host_of - 1 - copy_id) % host_count
    copied = owner * exp_host + plan_layer[host_of, copy_id]
    return jnp.where(local_id < exp_host, host_of * exp_host + local_id, copied)


def targets(experts_g, picks_g, table):
    flat_e = experts_g.reshape(-1)
    flat_p = picks_g.reshape(-1)
    matches = (table[None, :] == flat_e[:, None]).astype(jnp.int32)
    counts = jnp.sum(matches, axis=1)
    rank_in = jnp.cumsum(matches, axis=1) - 1
    wanted = flat_p % counts
    chosen = matches * (rank_in == wanted[:, None]).astype(jnp.int32)
    target = jnp.sum(chosen * jnp.arange(table.shape[0], dtype=jnp.int32)[None, :], axis=1)
    before = jnp.cumsum(chosen, axis=0) - chosen
    position = jnp.sum(before * chosen, axis=1)
    return (target, position)


def per_device(
    tokens,
    norm_gain,
    gate_weight,
    up_weight,
    down_weight,
    replica_plan,
    route_expert,
    replica_pick,
    combine_num,
):
    host_count = lax.axis_size("dp")
    host_index = lax.axis_index("dp")
    column_index = lax.axis_index("ep")
    layer_count = norm_gain.shape[0]
    width = norm_gain.shape[1]
    exp_host = gate_weight.shape[1]
    rep_host = replica_plan.shape[2]
    replicas = exp_host + rep_host
    group_rows = tokens.shape[0]
    top_count = route_expert.shape[2]
    capacity = group_rows // 2
    slice_width = tokens.shape[1]
    unit_count = gate_weight.shape[2]
    slot_count = host_count * capacity
    buffer_rows = host_count * replicas * capacity
    row_ids = jnp.arange(buffer_rows, dtype=jnp.int32)
    act_shape = (replicas, unit_count, host_count, capacity)
    stream = tokens
    update = jnp.zeros((group_rows, slice_width), jnp.float32)
    for layer_id in range(layer_count):
        extra = [
            replica_plan[layer_id, (host_index + 1 + copy_id) % host_count, copy_id]
            for copy_id in range(rep_host)
        ]
        chosen_ids = jnp.concatenate([jnp.arange(exp_host, dtype=jnp.int32), jnp.stack(extra)])
        gate_all = gate_weight[layer_id][chosen_ids]
        up_all = up_weight[layer_id][chosen_ids]
        down_all = down_weight[layer_id][chosen_ids]
        table = serve_table(replica_plan[layer_id], host_count, exp_host, rep_host)
        grouped_e = route_expert[layer_id].reshape(host_count, group_rows, top_count)
        grouped_p = replica_pick[layer_id].reshape(host_count, group_rows, top_count)
        every_target, every_position = jax.vmap(lambda e_blk, p_blk: targets(e_blk, p_blk, table))(
            grouped_e, grouped_p
        )
        owner_of = every_target // replicas
        slot_of = every_target % replicas
        destination_copy_id = jnp.clip(slot_of - exp_host, 0, rep_host - 1)
        moved = (owner_of - 1 - destination_copy_id) % host_count
        every_dest = jnp.where(slot_of < exp_host, owner_of, moved)
        every_slot = every_target % replicas
        dest = lax.dynamic_index_in_dim(every_dest, host_index, 0, keepdims=False)
        slot_of = lax.dynamic_index_in_dim(every_slot, host_index, 0, keepdims=False)
        position = lax.dynamic_index_in_dim(every_position, host_index, 0, keepdims=False)
        kept = position < capacity
        stream_f = stream.astype(jnp.float32)
        squares = lax.psum(jnp.sum(stream_f * stream_f, axis=1), "ep")
        inverse_rms = lax.rsqrt(squares / width + epsilon)
        gain_part = lax.dynamic_slice_in_dim(
            norm_gain[layer_id], column_index * slice_width, slice_width, 0
        )
        normed = (stream_f * inverse_rms[:, None] * gain_part[None, :]).astype(jnp.bfloat16)
        buffer_index = jnp.where(
            kept, dest * (replicas * capacity) + slot_of * capacity + position, -1
        ).reshape(group_rows, top_count)
        select = jnp.any(row_ids[:, None, None] == buffer_index[None, :, :], axis=2).astype(
            jnp.bfloat16
        )
        packed = jnp.dot(select, normed, preferred_element_type=jnp.float32).astype(jnp.bfloat16)
        packed = packed.reshape(host_count, replicas, capacity, slice_width)
        received = lax.all_to_all(packed, "dp", split_axis=0, concat_axis=0, tiled=True)
        portion = lax.all_gather(received, "ep", axis=3, tiled=True)
        gate_new = jnp.einsum(
            "srcd,rfd->rfsc", portion, gate_all, preferred_element_type=jnp.float32
        ).reshape(-1)
        up_new = jnp.einsum(
            "srcd,rfd->rfsc", portion, up_all, preferred_element_type=jnp.float32
        ).reshape(-1)
        gate_act = gate_new.reshape(act_shape)
        up_act = up_new.reshape(act_shape)
        hidden = (
            (jax.nn.silu(gate_act) * up_act)
            .astype(jnp.bfloat16)
            .reshape(replicas, unit_count, slot_count)
        )
        result = jnp.einsum(
            "rfs,rdf->rsd",
            lax.all_gather(hidden, "ep", axis=1, tiled=True),
            down_all,
            preferred_element_type=jnp.float32,
        ).reshape(-1)
        result = result.astype(jnp.bfloat16).reshape(replicas, host_count, capacity, slice_width)
        returned = lax.all_to_all(result, "dp", split_axis=1, concat_axis=1, tiled=True)
        flat_rows = returned.reshape(replicas * host_count * capacity, slice_width)
        row_pick = slot_of * slot_count + dest * capacity + jnp.minimum(position, capacity - 1)
        picked = flat_rows[row_pick].astype(jnp.float32).reshape(group_rows, top_count, slice_width)
        numerator = combine_num[layer_id].astype(jnp.float32)
        weights_k = numerator / jnp.sum(numerator, axis=1, keepdims=True)
        combine = weights_k * kept.reshape(group_rows, top_count).astype(jnp.float32)
        update = jnp.sum(combine[:, :, None] * picked, axis=1)
        stream = (stream_f + update).astype(jnp.bfloat16)
    return (stream, update.astype(jnp.bfloat16))


MESH_ID = pl.DeviceIdType.MESH
NT = (((1,), (1,)), ((), ()))
DIRECT = (1, 2, 4, 6)


def kernel(
    dims,
    plan_ref,
    tok_ref,
    gain_ref,
    route_ref,
    pick_ref,
    num_ref,
    gate_hbm,
    up_hbm,
    down_hbm,
    out_ref,
    last_ref,
    gate_buf,
    up_buf,
    down_buf,
    xg,
    xs,
    hid,
    cw,
    part_f,
    part_b,
    got,
    new_tok,
    gate_sem,
    up_sem,
    down_sem,
    z_send,
    z_recv,
    c_send,
    c_recv,
    p_send,
    p_recv,
    h_send,
    h_recv,
    r_send,
    r_recv,
):
    n_dp, layers, experts, rep, top, capacity = dims
    rows, width = tok_ref.shape
    units = gate_hbm.shape[2]
    features = gate_hbm.shape[3]
    f32 = jnp.float32
    me = lax.axis_index("ep")
    host = lax.axis_index("dp")
    bit_c = me % 2
    bit_x = (me // 2) % 2
    bit_y = me // 4

    def peer(rel):
        to = me
        if rel & 1:
            to = to + 1 - 2 * bit_c
        if rel & 2:
            to = to + 2 - 4 * bit_x
        if rel & 4:
            to = to + 4 - 8 * bit_y
        return to

    def fetch(hbm, buf, sem, layer, e, slot):
        return pltpu.make_async_copy(hbm.at[layer, e], buf.at[slot, e], sem.at[layer, e])

    for e in range(experts):
        fetch(gate_hbm, gate_buf, gate_sem, 0, e, 0).start()
        fetch(up_hbm, up_buf, up_sem, 0, e, 0).start()

    barrier = pltpu.get_barrier_semaphore()
    for k in range(1, n_dp):
        pl.semaphore_signal(
            barrier, inc=1, device_id={"dp": (host + k) % n_dp}, device_id_type=MESH_ID
        )
    for rel in range(1, 8):
        pl.semaphore_signal(barrier, inc=1, device_id={"ep": peer(rel)}, device_id_type=MESH_ID)
    pl.semaphore_wait(barrier, n_dp + 6)

    def block(layer, slot, group):
        lane = pl.multiple_of(slot * width, 128)
        row = pl.multiple_of(group * rows, rows)
        return xg.at[layer, pl.ds(row, rows), pl.ds(lane, width)]

    def z_copy(layer, src, k, group):
        return pltpu.make_async_remote_copy(
            src_ref=src,
            dst_ref=block(layer, me, group),
            send_sem=z_send.at[layer, k],
            recv_sem=z_recv.at[layer, k],
            device_id={"dp": (host + k) % n_dp},
            device_id_type=MESH_ID,
        )

    def p_copy(layer, k, slot, to, send, recv):
        ref = block(layer, slot, (host + n_dp - k) % n_dp)
        return pltpu.make_async_remote_copy(
            src_ref=ref,
            dst_ref=ref,
            send_sem=p_send.at[layer, k, send],
            recv_sem=p_recv.at[layer, k, recv],
            device_id={"ep": peer(to)},
            device_id_type=MESH_ID,
        )

    def c_copy(k, group):
        row = pl.multiple_of(group * rows, rows)
        ref = cw.at[:, pl.ds(row, rows), :]
        return pltpu.make_async_remote_copy(
            src_ref=ref,
            dst_ref=ref,
            send_sem=c_send.at[k],
            recv_sem=c_recv.at[k],
            device_id={"dp": (host + k) % n_dp},
            device_id_type=MESH_ID,
        )

    def h_copy(layer, e, slot, rel):
        lane = pl.multiple_of(slot * units, 128)
        ref = hid.at[layer, e, :, pl.ds(lane, units)]
        return pltpu.make_async_remote_copy(
            src_ref=ref,
            dst_ref=ref,
            send_sem=h_send.at[layer, e, rel],
            recv_sem=h_recv.at[layer, e, rel],
            device_id={"ep": peer(rel)},
            device_id_type=MESH_ID,
        )

    def r_copy(layer, k, group):
        row = pl.multiple_of(group * rows, rows)
        return pltpu.make_async_remote_copy(
            src_ref=part_b.at[layer, pl.ds(row, rows), :],
            dst_ref=got.at[layer, k],
            send_sem=r_send.at[layer, k],
            recv_sem=r_recv.at[layer, k],
            device_id={"dp": (host + k) % n_dp},
            device_id_type=MESH_ID,
        )

    def combine_weights(layer):
        count = rows * top
        reps = experts + rep
        pad = 32
        slot_t = lax.broadcasted_iota(jnp.int32, (pad, count), 0)
        table = (slot_t // reps) * experts + slot_t % reps
        for h in range(n_dp):
            for q in range(rep):
                base = ((h - 1 - q) % n_dp) * experts
                served = base + plan_ref[(layer * n_dp + h) * rep + q]
                table = jnp.where(slot_t == h * reps + experts + q, served, table)
        table = jnp.where(slot_t < n_dp * reps, table, -1)
        line = lax.broadcasted_iota(jnp.int32, route_ref.shape, 0) == layer * n_dp + host
        expert_of = jnp.sum(jnp.where(line, route_ref[...], 0), axis=0, keepdims=True)
        pick = jnp.sum(jnp.where(line, pick_ref[...], 0), axis=0, keepdims=True).astype(f32)
        which = lax.broadcasted_iota(jnp.int32, num_ref.shape, 0) == layer
        number = jnp.sum(jnp.where(which, num_ref[...], 0), axis=0, keepdims=True).astype(f32)
        matches = jnp.where(table == expert_of, 1.0, 0.0)
        counts = jnp.sum(matches, axis=0, keepdims=True)
        t_a = lax.broadcasted_iota(jnp.int32, (pad, pad), 0)
        t_b = lax.broadcasted_iota(jnp.int32, (pad, pad), 1)
        below = jnp.where(t_b < t_a, 1.0, 0.0)
        rank = jnp.dot(below, matches, preferred_element_type=f32)
        wanted = pick - counts * jnp.floor((pick + 0.5) / counts)
        chosen = matches * jnp.where(jnp.abs(rank - wanted) < 0.5, 1.0, 0.0)
        s_a = lax.broadcasted_iota(jnp.int32, (count, count), 0)
        s_b = lax.broadcasted_iota(jnp.int32, (count, count), 1)
        earlier = jnp.where(s_a < s_b, 1.0, 0.0)
        before = jnp.dot(chosen, earlier, preferred_element_type=f32)
        position = jnp.sum(before * chosen, axis=0, keepdims=True)
        same = jnp.where(s_a // top == s_b // top, 1.0, 0.0)
        number8 = jnp.broadcast_to(number, (8, count))
        total = jnp.dot(number8, same, preferred_element_type=f32)[0:1, :]
        weight = jnp.where(position < capacity - 0.5, number / total, 0.0)
        n_a = lax.broadcasted_iota(jnp.int32, (rows, count), 0)
        n_b = lax.broadcasted_iota(jnp.int32, (rows, count), 1)
        spread = jnp.where(n_b // top == n_a, weight, 0.0)
        e_a = lax.broadcasted_iota(jnp.int32, (128, count), 0)
        onehot = jnp.where(e_a == expert_of, 1.0, 0.0)
        row = pl.multiple_of(host * rows, rows)
        cw[layer, pl.ds(row, rows), :] = lax.dot_general(
            spread, onehot, NT, preferred_element_type=f32, precision=lax.Precision.HIGHEST
        )

    lane_w = pl.multiple_of(me * width, 128)
    row_h = pl.multiple_of(host * rows, rows)
    for layer in range(layers):
        src = tok_ref if layer == 0 else new_tok
        for k in range(1, n_dp):
            z_copy(layer, src, k, host).start()
        xg[layer, pl.ds(row_h, rows), pl.ds(lane_w, width)] = src[...]
        for i, rel in enumerate(DIRECT):
            p_copy(layer, 0, me, rel, i, rel - 1).start()
        if layer == 0:
            for e in range(experts):
                fetch(down_hbm, down_buf, down_sem, 0, e, 0).start()
            for later in range(1, layers):
                for e in range(experts):
                    fetch(gate_hbm, gate_buf, gate_sem, later, e, later).start()
                    fetch(up_hbm, up_buf, up_sem, later, e, later).start()
            for each in range(layers):
                combine_weights(each)
            for k in range(1, n_dp):
                c_copy(k, host).start()
        for k in range(1, n_dp):
            z_copy(layer, src, k, (host + n_dp - k) % n_dp).wait_recv()
            for i, rel in enumerate(DIRECT):
                p_copy(layer, k, me, rel, i, rel - 1).start()
        for k in range(n_dp):
            for i, rel in enumerate((2, 4, 6)):
                p_copy(layer, k, peer(rel), rel, 0, rel - 1).wait_recv()
                p_copy(layer, k, peer(rel), 1, 4 + i, rel).start()
        for k in range(n_dp):
            for rel in (1, 3, 5, 7):
                p_copy(layer, k, peer(rel), rel, 0, rel - 1).wait_recv()
        if layer == 0:
            for k in range(1, n_dp):
                c_copy(k, (host + n_dp - k) % n_dp).wait_recv()

        squares = jnp.zeros((n_dp * rows, 1), f32)
        for j in range(8):
            lane = slice(j * width, (j + 1) * width)
            x = xg[layer, :, lane].astype(f32)
            gained = x.reshape(-1, 8, width) * gain_ref[layer, :, lane][None]
            xs[:, lane] = gained.reshape(-1, width).astype(jnp.bfloat16)
            squares = squares + jnp.sum(x * x, axis=1, keepdims=True)
        inverse = lax.rsqrt(squares / features + epsilon)
        weights = cw[layer]
        column = lax.broadcasted_iota(jnp.int32, weights.shape, 1)

        def expert(e, carry):
            mine = jnp.where(column == host * experts + e, weights, 0.0)
            mine = jnp.sum(mine, axis=1, keepdims=True)
            fetch(gate_hbm, gate_buf, gate_sem, layer, e, layer).wait()
            gate = lax.dot_general(xs[...], gate_buf[layer, e], NT, preferred_element_type=f32)
            fetch(up_hbm, up_buf, up_sem, layer, e, layer).wait()
            up = lax.dot_general(xs[...], up_buf[layer, e], NT, preferred_element_type=f32)
            gate = gate * inverse
            hidden = gate / (1.0 + jnp.exp(-gate)) * (up * inverse) * mine
            lane = pl.multiple_of(me * units, 128)
            hid[layer, e, :, pl.ds(lane, units)] = hidden.astype(jnp.bfloat16)
            for rel in (6, 7, 2, 3, 4, 5, 1):
                h_copy(layer, e, me, rel).start()
            return carry

        lax.fori_loop(0, experts, expert, 0)
        part_f[...] = jnp.zeros_like(part_f)

        def project(e, carry):
            for rel in range(1, 8):
                h_copy(layer, e, peer(rel), rel).wait_recv()
            fetch(down_hbm, down_buf, down_sem, layer, e, 0).wait()
            part_f[...] += lax.dot_general(
                hid[layer, e], down_buf[0, e], NT, preferred_element_type=f32
            )
            if layer + 1 < layers:
                fetch(down_hbm, down_buf, down_sem, layer + 1, e, 0).start()
            return carry

        lax.fori_loop(0, experts, project, 0)
        part_b[layer] = part_f[...].astype(jnp.bfloat16)
        for k in range(1, n_dp):
            r_copy(layer, k, (host + k) % n_dp).start()
        update = part_f[pl.ds(row_h, rows), :]
        for k in range(1, n_dp):
            r_copy(layer, k, host).wait_recv()
        for k in range(1, n_dp):
            update = update + got[layer, k].astype(f32)
        stream = (src[...].astype(f32) + update).astype(jnp.bfloat16)
        if layer + 1 < layers:
            new_tok[...] = stream
        else:
            out_ref[...] = stream
            last_ref[...] = update.astype(jnp.bfloat16)

    for layer in range(layers):
        src = tok_ref if layer == 0 else new_tok
        for k in range(1, n_dp):
            z_copy(layer, src, k, host).wait_send()
            r_copy(layer, k, (host + k) % n_dp).wait_send()
        for k in range(n_dp):
            for i, rel in enumerate(DIRECT):
                p_copy(layer, k, me, rel, i, rel - 1).wait_send()
            for i, rel in enumerate((2, 4, 6)):
                p_copy(layer, k, peer(rel), 1, 4 + i, rel).wait_send()
        for e in range(experts):
            for rel in range(1, 8):
                h_copy(layer, e, me, rel).wait_send()
    for k in range(1, n_dp):
        c_copy(k, host).wait_send()


def fused(
    tokens,
    norm_gain,
    gate_weight,
    up_weight,
    down_weight,
    replica_plan,
    route_expert,
    replica_pick,
    combine_num,
):
    n_dp = lax.axis_size("dp")
    layers, features = norm_gain.shape
    rows, width = tokens.shape
    experts, units = gate_weight.shape[1:3]
    inner = down_weight.shape[3]
    rep = replica_plan.shape[2]
    top = route_expert.shape[2]
    count = n_dp * rows
    dims = (n_dp, layers, experts, rep, top, rows // 2)
    bf16 = jnp.bfloat16
    vmem = pl.BlockSpec(memory_space=pltpu.VMEM)
    dma = pltpu.SemaphoreType.DMA
    return pl.pallas_call(
        functools.partial(kernel, dims),
        out_shape=(
            jax.ShapeDtypeStruct((rows, width), bf16),
            jax.ShapeDtypeStruct((rows, width), bf16),
        ),
        in_specs=[pl.BlockSpec(memory_space=pltpu.SMEM)]
        + [vmem] * 5
        + [pl.BlockSpec(memory_space=pl.ANY)] * 3,
        out_specs=(vmem, vmem),
        scratch_shapes=[
            pltpu.VMEM((layers, experts, units, features), bf16),
            pltpu.VMEM((layers, experts, units, features), bf16),
            pltpu.VMEM((1, experts, width, inner), bf16),
            pltpu.VMEM((layers, count, features), bf16),
            pltpu.VMEM((count, features), bf16),
            pltpu.VMEM((layers, experts, count, inner), bf16),
            pltpu.VMEM((layers, count, 128), jnp.float32),
            pltpu.VMEM((count, width), jnp.float32),
            pltpu.VMEM((layers, count, width), bf16),
            pltpu.VMEM((layers, n_dp, rows, width), bf16),
            pltpu.VMEM((rows, width), bf16),
            dma((layers, experts)),
            dma((layers, experts)),
            dma((layers, experts)),
            dma((layers, n_dp)),
            dma((layers, n_dp)),
            dma((n_dp,)),
            dma((n_dp,)),
            dma((layers, n_dp, 7)),
            dma((layers, n_dp, 7)),
            dma((layers, experts, 8)),
            dma((layers, experts, 8)),
            dma((layers, n_dp)),
            dma((layers, n_dp)),
        ],
        compiler_params=pltpu.CompilerParams(
            collective_id=0, has_side_effects=True, vmem_limit_bytes=67043328
        ),
        name="moe_layers",
    )(
        replica_plan.reshape(-1),
        tokens,
        jnp.broadcast_to(norm_gain[:, None, :], (layers, 8, features)),
        route_expert.reshape(layers * n_dp, rows * top),
        replica_pick.reshape(layers * n_dp, rows * top),
        jnp.pad(combine_num.reshape(layers, rows * top), ((0, -layers % 8), (0, 0))),
        gate_weight,
        up_weight,
        down_weight,
    )


def device_step(*arrays):
    tokens, gate_weight, route_expert = arrays[0], arrays[2], arrays[6]
    rows, width = tokens.shape
    fits = (
        lax.axis_size("ep") == 8
        and width % 128 == 0
        and gate_weight.shape[2] % 128 == 0
        and rows % 16 == 0
        and rows * route_expert.shape[2] == 128
    )
    return fused(*arrays) if fits else per_device(*arrays)


def solution(mesh):
    return jax.shard_map(
        device_step,
        mesh=mesh,
        in_specs=(
            P("dp", "ep"),
            P(),
            P(None, "dp", "ep", None),
            P(None, "dp", "ep", None),
            P(None, "dp", "ep", None),
            P(),
            P(),
            P(),
            P(None, "dp", None),
        ),
        out_specs=(P("dp", "ep"), P("dp", "ep")),
        check_vma=False,
    )
```

```python
import jax
import jax.numpy as jnp
from jax import lax
from jax.experimental import pallas as pl
from jax.experimental.pallas import tpu as pltpu
from jax.sharding import PartitionSpec as P

import functools

epsilon = 1e-06


def serve_table(plan_layer, host_count, exp_host, rep_host):
    replicas = exp_host + rep_host
    flat_ids = jnp.arange(host_count * replicas, dtype=jnp.int32)
    host_of = flat_ids // replicas
    local_id = flat_ids % replicas
    copy_id = jnp.clip(local_id - exp_host, 0, rep_host - 1)
    owner = (host_of - 1 - copy_id) % host_count
    copied = owner * exp_host + plan_layer[host_of, copy_id]
    return jnp.where(local_id < exp_host, host_of * exp_host + local_id, copied)


def targets(experts_g, picks_g, table):
    flat_e = experts_g.reshape(-1)
    flat_p = picks_g.reshape(-1)
    matches = (table[None, :] == flat_e[:, None]).astype(jnp.int32)
    counts = jnp.sum(matches, axis=1)
    rank_in = jnp.cumsum(matches, axis=1) - 1
    wanted = flat_p % counts
    chosen = matches * (rank_in == wanted[:, None]).astype(jnp.int32)
    target = jnp.sum(chosen * jnp.arange(table.shape[0], dtype=jnp.int32)[None, :], axis=1)
    before = jnp.cumsum(chosen, axis=0) - chosen
    position = jnp.sum(before * chosen, axis=1)
    return (target, position)


def per_device(
    tokens,
    norm_gain,
    gate_weight,
    up_weight,
    down_weight,
    replica_plan,
    route_expert,
    replica_pick,
    combine_num,
):
    host_count = lax.axis_size("dp")
    host_index = lax.axis_index("dp")
    column_index = lax.axis_index("ep")
    layer_count = norm_gain.shape[0]
    width = norm_gain.shape[1]
    exp_host = gate_weight.shape[1]
    rep_host = replica_plan.shape[2]
    replicas = exp_host + rep_host
    group_rows = tokens.shape[0]
    top_count = route_expert.shape[2]
    capacity = group_rows // 2
    slice_width = tokens.shape[1]
    unit_count = gate_weight.shape[2]
    slot_count = host_count * capacity
    buffer_rows = host_count * replicas * capacity
    row_ids = jnp.arange(buffer_rows, dtype=jnp.int32)
    act_shape = (replicas, unit_count, host_count, capacity)
    stream = tokens
    update = jnp.zeros((group_rows, slice_width), jnp.float32)
    for layer_id in range(layer_count):
        extra = [
            replica_plan[layer_id, (host_index + 1 + copy_id) % host_count, copy_id]
            for copy_id in range(rep_host)
        ]
        chosen_ids = jnp.concatenate([jnp.arange(exp_host, dtype=jnp.int32), jnp.stack(extra)])
        gate_all = gate_weight[layer_id][chosen_ids]
        up_all = up_weight[layer_id][chosen_ids]
        down_all = down_weight[layer_id][chosen_ids]
        table = serve_table(replica_plan[layer_id], host_count, exp_host, rep_host)
        grouped_e = route_expert[layer_id].reshape(host_count, group_rows, top_count)
        grouped_p = replica_pick[layer_id].reshape(host_count, group_rows, top_count)
        every_target, every_position = jax.vmap(lambda e_blk, p_blk: targets(e_blk, p_blk, table))(
            grouped_e, grouped_p
        )
        owner_of = every_target // replicas
        slot_of = every_target % replicas
        destination_copy_id = jnp.clip(slot_of - exp_host, 0, rep_host - 1)
        moved = (owner_of - 1 - destination_copy_id) % host_count
        every_dest = jnp.where(slot_of < exp_host, owner_of, moved)
        every_slot = every_target % replicas
        dest = lax.dynamic_index_in_dim(every_dest, host_index, 0, keepdims=False)
        slot_of = lax.dynamic_index_in_dim(every_slot, host_index, 0, keepdims=False)
        position = lax.dynamic_index_in_dim(every_position, host_index, 0, keepdims=False)
        kept = position < capacity
        stream_f = stream.astype(jnp.float32)
        squares = lax.psum(jnp.sum(stream_f * stream_f, axis=1), "ep")
        inverse_rms = lax.rsqrt(squares / width + epsilon)
        gain_part = lax.dynamic_slice_in_dim(
            norm_gain[layer_id], column_index * slice_width, slice_width, 0
        )
        normed = (stream_f * inverse_rms[:, None] * gain_part[None, :]).astype(jnp.bfloat16)
        buffer_index = jnp.where(
            kept, dest * (replicas * capacity) + slot_of * capacity + position, -1
        ).reshape(group_rows, top_count)
        select = jnp.any(row_ids[:, None, None] == buffer_index[None, :, :], axis=2).astype(
            jnp.bfloat16
        )
        packed = jnp.dot(select, normed, preferred_element_type=jnp.float32).astype(jnp.bfloat16)
        packed = packed.reshape(host_count, replicas, capacity, slice_width)
        received = lax.all_to_all(packed, "dp", split_axis=0, concat_axis=0, tiled=True)
        portion = lax.all_gather(received, "ep", axis=3, tiled=True)
        gate_new = jnp.einsum(
            "srcd,rfd->rfsc", portion, gate_all, preferred_element_type=jnp.float32
        ).reshape(-1)
        up_new = jnp.einsum(
            "srcd,rfd->rfsc", portion, up_all, preferred_element_type=jnp.float32
        ).reshape(-1)
        gate_act = gate_new.reshape(act_shape)
        up_act = up_new.reshape(act_shape)
        hidden = (
            (jax.nn.silu(gate_act) * up_act)
            .astype(jnp.bfloat16)
            .reshape(replicas, unit_count, slot_count)
        )
        result = jnp.einsum(
            "rfs,rdf->rsd",
            lax.all_gather(hidden, "ep", axis=1, tiled=True),
            down_all,
            preferred_element_type=jnp.float32,
        ).reshape(-1)
        result = result.astype(jnp.bfloat16).reshape(replicas, host_count, capacity, slice_width)
        returned = lax.all_to_all(result, "dp", split_axis=1, concat_axis=1, tiled=True)
        flat_rows = returned.reshape(replicas * host_count * capacity, slice_width)
        row_pick = slot_of * slot_count + dest * capacity + jnp.minimum(position, capacity - 1)
        picked = flat_rows[row_pick].astype(jnp.float32).reshape(group_rows, top_count, slice_width)
        numerator = combine_num[layer_id].astype(jnp.float32)
        weights_k = numerator / jnp.sum(numerator, axis=1, keepdims=True)
        combine = weights_k * kept.reshape(group_rows, top_count).astype(jnp.float32)
        update = jnp.sum(combine[:, :, None] * picked, axis=1)
        stream = (stream_f + update).astype(jnp.bfloat16)
    return (stream, update.astype(jnp.bfloat16))


MESH_ID = pl.DeviceIdType.MESH
NT = (((1,), (1,)), ((), ()))
DIRECT = (1, 2, 4, 6)


def kernel(
    dims,
    plan_ref,
    tok_ref,
    gain_ref,
    ints_ref,
    gate_hbm,
    up_hbm,
    down_hbm,
    out_ref,
    last_ref,
    gate_buf,
    up_buf,
    down_buf,
    xg,
    xs,
    hid,
    cw,
    part_f,
    part_b,
    got,
    new_tok,
    gate_sem,
    up_sem,
    down_sem,
    z_send,
    z_recv,
    c_send,
    c_recv,
    p_send,
    p_recv,
    h_send,
    h_recv,
    r_send,
    r_recv,
):
    n_dp, layers, experts, rep, top, capacity = dims
    rows, width = tok_ref.shape
    units = gate_hbm.shape[2]
    features = gate_hbm.shape[3]
    f32 = jnp.float32
    me = lax.axis_index("ep")
    host = lax.axis_index("dp")
    bit_c = me % 2
    bit_x = (me // 2) % 2
    bit_y = me // 4

    def peer(rel):
        to = me
        if rel & 1:
            to = to + 1 - 2 * bit_c
        if rel & 2:
            to = to + 2 - 4 * bit_x
        if rel & 4:
            to = to + 4 - 8 * bit_y
        return to

    def fetch(hbm, buf, sem, layer, e, slot):
        return pltpu.make_async_copy(hbm.at[layer, e], buf.at[slot, e], sem.at[layer, e])

    for e in range(experts):
        fetch(gate_hbm, gate_buf, gate_sem, 0, e, 0).start()
        fetch(up_hbm, up_buf, up_sem, 0, e, 0).start()

    barrier = pltpu.get_barrier_semaphore()
    for k in range(1, n_dp):
        pl.semaphore_signal(
            barrier, inc=1, device_id={"dp": (host + k) % n_dp}, device_id_type=MESH_ID
        )
    for rel in range(1, 8):
        pl.semaphore_signal(barrier, inc=1, device_id={"ep": peer(rel)}, device_id_type=MESH_ID)
    pl.semaphore_wait(barrier, n_dp + 6)

    def block(layer, slot, group):
        lane = pl.multiple_of(slot * width, 128)
        row = pl.multiple_of(group * rows, rows)
        return xg.at[layer, pl.ds(row, rows), pl.ds(lane, width)]

    def z_copy(layer, src, k, group):
        return pltpu.make_async_remote_copy(
            src_ref=src,
            dst_ref=block(layer, me, group),
            send_sem=z_send.at[layer, k],
            recv_sem=z_recv.at[layer, k],
            device_id={"dp": (host + k) % n_dp},
            device_id_type=MESH_ID,
        )

    def p_copy(layer, k, slot, to, send, recv):
        ref = block(layer, slot, (host + n_dp - k) % n_dp)
        return pltpu.make_async_remote_copy(
            src_ref=ref,
            dst_ref=ref,
            send_sem=p_send.at[layer, k, send],
            recv_sem=p_recv.at[layer, k, recv],
            device_id={"ep": peer(to)},
            device_id_type=MESH_ID,
        )

    def c_copy(k, group):
        row = pl.multiple_of(group * rows, rows)
        ref = cw.at[:, pl.ds(row, rows), :]
        return pltpu.make_async_remote_copy(
            src_ref=ref,
            dst_ref=ref,
            send_sem=c_send.at[k],
            recv_sem=c_recv.at[k],
            device_id={"dp": (host + k) % n_dp},
            device_id_type=MESH_ID,
        )

    def h_copy(layer, e, slot, rel):
        lane = pl.multiple_of(slot * units, 128)
        ref = hid.at[layer, e, :, pl.ds(lane, units)]
        return pltpu.make_async_remote_copy(
            src_ref=ref,
            dst_ref=ref,
            send_sem=h_send.at[layer, e, rel],
            recv_sem=h_recv.at[layer, e, rel],
            device_id={"ep": peer(rel)},
            device_id_type=MESH_ID,
        )

    def r_copy(layer, k, group):
        row = pl.multiple_of(group * rows, rows)
        return pltpu.make_async_remote_copy(
            src_ref=part_b.at[layer, pl.ds(row, rows), :],
            dst_ref=got.at[layer, k],
            send_sem=r_send.at[layer, k],
            recv_sem=r_recv.at[layer, k],
            device_id={"dp": (host + k) % n_dp},
            device_id_type=MESH_ID,
        )

    def combine_weights(layer):
        count = rows * top
        reps = experts + rep
        pad = 32
        slot_t = lax.broadcasted_iota(jnp.int32, (pad, count), 0)
        table = (slot_t // reps) * experts + slot_t % reps
        for h in range(n_dp):
            for q in range(rep):
                base = ((h - 1 - q) % n_dp) * experts
                served = base + plan_ref[(layer * n_dp + h) * rep + q]
                table = jnp.where(slot_t == h * reps + experts + q, served, table)
        table = jnp.where(slot_t < n_dp * reps, table, -1)
        lines = layers * n_dp
        row_of = lax.broadcasted_iota(jnp.int32, (lines, count), 0)
        line = row_of == layer * n_dp + host
        routes, picks = ints_ref[0:lines, :], ints_ref[lines : 2 * lines, :]
        numbers = ints_ref[2 * lines : 3 * lines, :]
        expert_of = jnp.sum(jnp.where(line, routes, 0), axis=0, keepdims=True)
        pick = jnp.sum(jnp.where(line, picks, 0), axis=0, keepdims=True).astype(f32)
        number = jnp.sum(jnp.where(row_of == layer, numbers, 0), axis=0, keepdims=True)
        number = number.astype(f32)
        matches = jnp.where(table == expert_of, 1.0, 0.0)
        counts = jnp.sum(matches, axis=0, keepdims=True)
        t_a = lax.broadcasted_iota(jnp.int32, (pad, pad), 0)
        t_b = lax.broadcasted_iota(jnp.int32, (pad, pad), 1)
        below = jnp.where(t_b < t_a, 1.0, 0.0)
        rank = jnp.dot(below, matches, preferred_element_type=f32)
        wanted = pick - counts * jnp.floor((pick + 0.5) / counts)
        chosen = matches * jnp.where(jnp.abs(rank - wanted) < 0.5, 1.0, 0.0)
        s_a = lax.broadcasted_iota(jnp.int32, (count, count), 0)
        s_b = lax.broadcasted_iota(jnp.int32, (count, count), 1)
        earlier = jnp.where(s_a < s_b, 1.0, 0.0)
        before = jnp.dot(chosen, earlier, preferred_element_type=f32)
        position = jnp.sum(before * chosen, axis=0, keepdims=True)
        same = jnp.where(s_a // top == s_b // top, 1.0, 0.0)
        number8 = jnp.broadcast_to(number, (8, count))
        total = jnp.dot(number8, same, preferred_element_type=f32)[0:1, :]
        weight = jnp.where(position < capacity - 0.5, number / total, 0.0)
        n_a = lax.broadcasted_iota(jnp.int32, (rows, count), 0)
        n_b = lax.broadcasted_iota(jnp.int32, (rows, count), 1)
        spread = jnp.where(n_b // top == n_a, weight, 0.0)
        e_a = lax.broadcasted_iota(jnp.int32, (128, count), 0)
        onehot = jnp.where(e_a == expert_of, 1.0, 0.0)
        row = pl.multiple_of(host * rows, rows)
        cw[layer, pl.ds(row, rows), :] = lax.dot_general(
            spread, onehot, NT, preferred_element_type=f32, precision=lax.Precision.HIGHEST
        )

    lane_w = pl.multiple_of(me * width, 128)
    row_h = pl.multiple_of(host * rows, rows)
    for layer in range(layers):
        src = tok_ref if layer == 0 else new_tok
        for k in range(1, n_dp):
            z_copy(layer, src, k, host).start()
        xg[layer, pl.ds(row_h, rows), pl.ds(lane_w, width)] = src[...]
        for i, rel in enumerate(DIRECT):
            p_copy(layer, 0, me, rel, i, rel - 1).start()
        if layer == 0:
            for e in range(experts):
                fetch(down_hbm, down_buf, down_sem, 0, e, 0).start()
            for later in range(1, layers):
                for e in range(experts):
                    fetch(gate_hbm, gate_buf, gate_sem, later, e, later).start()
                    fetch(up_hbm, up_buf, up_sem, later, e, later).start()
        for k in range(1, n_dp):
            z_copy(layer, src, k, (host + n_dp - k) % n_dp).wait_recv()
            for i, rel in enumerate(DIRECT):
                p_copy(layer, k, me, rel, i, rel - 1).start()
        for k in range(n_dp):
            for i, rel in enumerate((2, 4, 6)):
                p_copy(layer, k, peer(rel), rel, 0, rel - 1).wait_recv()
                p_copy(layer, k, peer(rel), 1, 4 + i, rel).start()
        if layer == 0:
            for each in range(layers):
                combine_weights(each)
            for k in range(1, n_dp):
                c_copy(k, host).start()
        for k in range(n_dp):
            for rel in (1, 3, 5, 7):
                p_copy(layer, k, peer(rel), rel, 0, rel - 1).wait_recv()
        if layer == 0:
            for k in range(1, n_dp):
                c_copy(k, (host + n_dp - k) % n_dp).wait_recv()

        squares = jnp.zeros((n_dp * rows, 1), f32)
        for j in range(8):
            lane = slice(j * width, (j + 1) * width)
            x = xg[layer, :, lane].astype(f32)
            gained = x.reshape(-1, 8, width) * gain_ref[layer, :, lane][None]
            xs[:, lane] = gained.reshape(-1, width).astype(jnp.bfloat16)
            squares = squares + jnp.sum(x * x, axis=1, keepdims=True)
        inverse = lax.rsqrt(squares / features + epsilon)
        weights = cw[layer]
        column = lax.broadcasted_iota(jnp.int32, weights.shape, 1)

        def expert(e, carry):
            mine = jnp.where(column == host * experts + e, weights, 0.0)
            mine = jnp.sum(mine, axis=1, keepdims=True)
            fetch(gate_hbm, gate_buf, gate_sem, layer, e, layer).wait()
            gate = lax.dot_general(xs[...], gate_buf[layer, e], NT, preferred_element_type=f32)
            fetch(up_hbm, up_buf, up_sem, layer, e, layer).wait()
            up = lax.dot_general(xs[...], up_buf[layer, e], NT, preferred_element_type=f32)
            gate = gate * inverse
            hidden = gate / (1.0 + jnp.exp(-gate)) * (up * inverse) * mine
            lane = pl.multiple_of(me * units, 128)
            hid[layer, e, :, pl.ds(lane, units)] = hidden.astype(jnp.bfloat16)
            for rel in (6, 7, 2, 3, 4, 5, 1):
                h_copy(layer, e, me, rel).start()
            return carry

        lax.fori_loop(0, experts, expert, 0)
        part_f[...] = jnp.zeros_like(part_f)

        def project(e, carry):
            for rel in range(1, 8):
                h_copy(layer, e, peer(rel), rel).wait_recv()
            fetch(down_hbm, down_buf, down_sem, layer, e, 0).wait()
            part_f[...] += lax.dot_general(
                hid[layer, e], down_buf[0, e], NT, preferred_element_type=f32
            )
            if layer + 1 < layers:
                fetch(down_hbm, down_buf, down_sem, layer + 1, e, 0).start()
            return carry

        lax.fori_loop(0, experts, project, 0)
        part_b[layer] = part_f[...].astype(jnp.bfloat16)
        for k in range(1, n_dp):
            r_copy(layer, k, (host + k) % n_dp).start()
        update = part_f[pl.ds(row_h, rows), :]
        for k in range(1, n_dp):
            r_copy(layer, k, host).wait_recv()
        for k in range(1, n_dp):
            update = update + got[layer, k].astype(f32)
        stream = (src[...].astype(f32) + update).astype(jnp.bfloat16)
        if layer + 1 < layers:
            new_tok[...] = stream
        else:
            out_ref[...] = stream
            last_ref[...] = update.astype(jnp.bfloat16)

    for layer in range(layers):
        src = tok_ref if layer == 0 else new_tok
        for k in range(1, n_dp):
            z_copy(layer, src, k, host).wait_send()
            r_copy(layer, k, (host + k) % n_dp).wait_send()
        for k in range(n_dp):
            for i, rel in enumerate(DIRECT):
                p_copy(layer, k, me, rel, i, rel - 1).wait_send()
            for i, rel in enumerate((2, 4, 6)):
                p_copy(layer, k, peer(rel), 1, 4 + i, rel).wait_send()
        for e in range(experts):
            for rel in range(1, 8):
                h_copy(layer, e, me, rel).wait_send()
    for k in range(1, n_dp):
        c_copy(k, host).wait_send()


def fused(
    tokens,
    norm_gain,
    gate_weight,
    up_weight,
    down_weight,
    replica_plan,
    route_expert,
    replica_pick,
    combine_num,
):
    n_dp = lax.axis_size("dp")
    layers, features = norm_gain.shape
    rows, width = tokens.shape
    experts, units = gate_weight.shape[1:3]
    inner = down_weight.shape[3]
    rep = replica_plan.shape[2]
    top = route_expert.shape[2]
    count = n_dp * rows
    dims = (n_dp, layers, experts, rep, top, rows // 2)
    bf16 = jnp.bfloat16
    lines = layers * n_dp
    own = combine_num.reshape(layers, rows * top)
    ints = jnp.concatenate(
        [
            route_expert.reshape(lines, rows * top),
            replica_pick.reshape(lines, rows * top),
            jnp.pad(own, ((0, lines - layers), (0, 0))),
        ]
    )
    vmem = pl.BlockSpec(memory_space=pltpu.VMEM)
    dma = pltpu.SemaphoreType.DMA
    return pl.pallas_call(
        functools.partial(kernel, dims),
        out_shape=(
            jax.ShapeDtypeStruct((rows, width), bf16),
            jax.ShapeDtypeStruct((rows, width), bf16),
        ),
        in_specs=[pl.BlockSpec(memory_space=pltpu.SMEM)]
        + [vmem] * 3
        + [pl.BlockSpec(memory_space=pl.ANY)] * 3,
        out_specs=(vmem, vmem),
        scratch_shapes=[
            pltpu.VMEM((layers, experts, units, features), bf16),
            pltpu.VMEM((layers, experts, units, features), bf16),
            pltpu.VMEM((1, experts, width, inner), bf16),
            pltpu.VMEM((layers, count, features), bf16),
            pltpu.VMEM((count, features), bf16),
            pltpu.VMEM((layers, experts, count, inner), bf16),
            pltpu.VMEM((layers, count, 128), jnp.float32),
            pltpu.VMEM((count, width), jnp.float32),
            pltpu.VMEM((layers, count, width), bf16),
            pltpu.VMEM((layers, n_dp, rows, width), bf16),
            pltpu.VMEM((rows, width), bf16),
            dma((layers, experts)),
            dma((layers, experts)),
            dma((layers, experts)),
            dma((layers, n_dp)),
            dma((layers, n_dp)),
            dma((n_dp,)),
            dma((n_dp,)),
            dma((layers, n_dp, 7)),
            dma((layers, n_dp, 7)),
            dma((layers, experts, 8)),
            dma((layers, experts, 8)),
            dma((layers, n_dp)),
            dma((layers, n_dp)),
        ],
        compiler_params=pltpu.CompilerParams(
            collective_id=0, has_side_effects=True, vmem_limit_bytes=67043328
        ),
        name="moe_layers",
    )(
        replica_plan.reshape(-1),
        tokens,
        jnp.broadcast_to(norm_gain[:, None, :], (layers, 8, features)),
        ints,
        gate_weight,
        up_weight,
        down_weight,
    )


def device_step(*arrays):
    tokens, gate_weight, route_expert = arrays[0], arrays[2], arrays[6]
    rows, width = tokens.shape
    fits = (
        lax.axis_size("ep") == 8
        and width % 128 == 0
        and gate_weight.shape[2] % 128 == 0
        and rows % 16 == 0
        and arrays[1].shape[0] * lax.axis_size("dp") % 8 == 0
        and rows * route_expert.shape[2] == 128
    )
    return fused(*arrays) if fits else per_device(*arrays)


def solution(mesh):
    return jax.shard_map(
        device_step,
        mesh=mesh,
        in_specs=(
            P("dp", "ep"),
            P(),
            P(None, "dp", "ep", None),
            P(None, "dp", "ep", None),
            P(None, "dp", "ep", None),
            P(),
            P(),
            P(),
            P(None, "dp", None),
        ),
        out_specs=(P("dp", "ep"), P("dp", "ep")),
        check_vma=False,
    )
```
